32 devices in a mesh: data: 1 (over z), expert: 32 (over y, x, core).
Axes of the slice: x: 4, y: 4, z: 1, core: 2. Of those that a mesh axis runs over, the one named last changes fastest.
The devices are a block of a 4x4x8 slice.
Arguments:
- x: bfloat16 [8192, 2048], P(('data', 'expert'))
- idx: int32 [8192, 8], P(('data', 'expert'))
- g: float32 [8192, 8], P(('data', 'expert'))
- hot_tok: int32 [1024], P(('data', 'expert'))
- W1: bfloat16 [128, 2048, 768], P('expert')
- W3: bfloat16 [128, 2048, 768], P('expert')
- W2: bfloat16 [128, 768, 2048], P('expert')
Outputs:
- output: bfloat16 [8192, 2048], P(('data', 'expert'))
All inputs are finite; a program needn't handle non-finite values.
Results may differ from the reference program's by a relative error of at most 0.001.
Values are sent between devices in bfloat16 or wider.
A program may use at most 768 MiB of HBM per device.

```python
import jax
import jax.numpy as jnp
from jax import lax

EXPERTS = 128
TOP = 8
D = 2048
FF = 768
TOKENS = 256
HOT_DIV = 8
GROUP = 32

HOT_CAP = TOKENS // HOT_DIV
COLD_CAP = 2 * ((TOKENS * TOP - HOT_CAP + EXPERTS - 2) // (EXPERTS - 1))


def _weights(key, e, fan_in, fan_out):
    keys = jax.random.split(key, e)
    return lax.map(lambda k: (jax.random.normal(k, (fan_in, fan_out), jnp.float32) * fan_in ** -0.5).astype(jnp.bfloat16), keys)


def _chip_ids(key):
    k1, k2, k3 = jax.random.split(key, 3)
    t = jnp.arange(TOKENS)[:, None]
    j = jnp.arange(TOP)[None, :]
    hot = (t < HOT_CAP) & (j == 0)
    c = jnp.where(t < HOT_CAP, t * (TOP - 1) + j - 1, HOT_CAP * (TOP - 1) + (t - HOT_CAP) * TOP + j)
    seq = jnp.concatenate([jnp.arange(EXPERTS - 1), jnp.arange((EXPERTS - 1) // 2)])
    m = EXPERTS - 1 + (EXPERTS - 1) // 2
    off = jax.random.randint(k1, (), 0, m)
    perm = jax.random.permutation(k2, EXPERTS - 1)
    ids = jnp.flip(jnp.where(hot, 0, 1 + perm[seq[(c + off) % m]]), axis=1)
    shift = jax.random.randint(k3, (), 0, TOKENS)
    ids = jnp.roll(ids, shift, axis=0)
    hot_tok = jnp.sort((jnp.arange(HOT_CAP) + shift) % TOKENS)
    return ids.astype(jnp.int32), hot_tok.astype(jnp.int32)


def setup_inputs(seed: int = 0, part: int = 0) -> dict:
    kdata, kw = jax.random.split(jax.random.PRNGKey(seed))
    kx, kr, kg = jax.random.split(jax.random.fold_in(kdata, part), 3)
    k1, k3, k2 = jax.random.split(kw, 3)
    x = jax.random.normal(kx, (GROUP * TOKENS, D), jnp.float32).astype(jnp.bfloat16)
    ids, hot = jax.vmap(_chip_ids)(jax.random.split(jax.random.fold_in(kr, 7), GROUP))
    idx = ids.reshape(GROUP * TOKENS, TOP)
    u = jax.random.uniform(kg, (GROUP * TOKENS, TOP), jnp.float32)
    g = jnp.where(idx == 0, 0.6 + 0.4 * u, 0.2 + 0.5 * u)
    return {
        'x': x,
        'idx': idx,
        'g': g,
        'hot_tok': hot.reshape(GROUP * HOT_CAP),
        'W1': _weights(k1, EXPERTS, D, FF),
        'W3': _weights(k3, EXPERTS, D, FF),
        'W2': _weights(k2, EXPERTS, FF, D),
    }


def _expert(xr, w1, w3, w2):
    a = jnp.dot(xr, w1, preferred_element_type=jnp.float32)
    b = jnp.dot(xr, w3, preferred_element_type=jnp.float32)
    u = (jax.nn.silu(a) * b).astype(jnp.bfloat16)
    return jnp.dot(u, w2, preferred_element_type=jnp.float32).astype(jnp.bfloat16)


def reference(x, idx, g, hot_tok, W1, W3, W2):
    gate = jnp.where(idx == 0, g, 0.0).sum(axis=1)
    rows = (jnp.arange(GROUP)[:, None] * TOKENS + hot_tok.reshape(GROUP, HOT_CAP)).reshape(-1)
    hh = _expert(x[rows], W1[0], W3[0], W2[0]).astype(jnp.float32)
    y = jnp.zeros((GROUP * TOKENS, D), jnp.float32).at[rows].add(gate[rows][:, None] * hh)
    flat = idx.reshape(-1)
    order = jnp.argsort(flat, stable=True)
    counts = jnp.bincount(flat, length=EXPERTS)
    starts = jnp.cumsum(counts) - counts
    cap = GROUP * COLD_CAP
    order = jnp.concatenate([order, jnp.zeros((cap,), order.dtype)])
    gflat = g.reshape(-1)

    def step(y, ew):
        e, w1, w3, w2 = ew
        r = lax.dynamic_slice(order, (starts[e],), (cap,))
        valid = jnp.arange(cap) < counts[e]
        he = _expert(x[r // TOP], w1, w3, w2).astype(jnp.float32)
        return y.at[r // TOP].add(jnp.where(valid[:, None], gflat[r][:, None] * he, 0.0)), None

    y, _ = lax.scan(step, y, (jnp.arange(1, EXPERTS), W1[1:], W3[1:], W2[1:]))
    return y.astype(jnp.bfloat16)
```

```python
import functools
import math

import jax
import jax.numpy as jnp
from jax import lax
from jax.experimental import pallas as pl
from jax.experimental.pallas import tpu as pltpu
from jax.sharding import PartitionSpec as P

MESH = pl.DeviceIdType.MESH
F32 = jnp.float32
BF16 = jnp.bfloat16
ND = 4


def _where(n):
    me = lax.axis_index('expert')
    c = me % 2
    chip = me // 2
    return me, c, chip % ND, chip // ND


def _chip(k, p, q):
    p = p % ND
    q = q % ND
    return (1 - k) * (q * ND + p) + k * (p * ND + q)


def _near(j):
    return j + j // 2 - 2 * (j // 3)


def _greet(devs):
    bar = pltpu.get_barrier_semaphore()
    for dev in devs:
        pl.semaphore_signal(bar, inc=1, device_id={'expert': dev}, device_id_type=MESH)
    pl.semaphore_wait(bar, len(devs))


def _dispatch_kernel(n, el, cap, x_ref, meta_ref, w1_ref, w3_ref, w2_ref, h_ref, xall,
                     w1v, w3v, w2v, xb, xg, uv, hb, wsem, bsem, osem, ssem, rsem):
    t, d = x_ref.shape
    f = w1v.shape[2]
    r = el * cap
    me, c, cx, cy = _where(n)
    o = 1 - c
    p = o * cx + c * cy
    q = o * cy + c * cx
    partner = me + 1 - 2 * c

    def dev(pp, qq):
        return _chip(c, pp, qq) * 2 + c

    _greet([dev(p + 1, q), dev(p - 1, q), dev(p, q + 1), dev(p, q - 1), partner])

    loads = []
    for i, (a, b) in enumerate(((w1_ref, w1v), (w3_ref, w3v), (w2_ref, w2v))):
        loads.append(pltpu.make_async_copy(a, b, wsem.at[i]))
    sends = []

    def part(ref, half):
        return ref if half is None else ref.at[pl.ds(half * (t // 2), t // 2)]

    def send(b, ref, half, to):
        cp = pltpu.make_async_remote_copy(
            src_ref=part(ref, half), dst_ref=part(xall.at[b], half), send_sem=ssem.at[len(sends)],
            recv_sem=rsem.at[b, half or 0], device_id={'expert': to}, device_id_type=MESH)
        cp.start()
        sends.append(cp)

    def arrived(b, half):
        pltpu.make_async_remote_copy(
            src_ref=part(xall.at[b], half), dst_ref=part(xall.at[b], half), send_sem=ssem.at[0],
            recv_sem=rsem.at[b, half or 0], device_id={'expert': partner}, device_id_type=MESH).wait_recv()

    for to in (dev(p + 1, q), dev(p - 1, q), dev(p, q + 1), dev(p, q - 1), partner):
        send(me, x_ref, None, to)
    for cp in loads:
        cp.start()

    def spread(b):
        for to in (dev(p, q + 1), dev(p, q - 1), partner):
            send(b, xall.at[b], None, to)

    b = dev(p + 1, q)
    arrived(b, None)
    send(b, xall.at[b], 1, dev(p - 1, q))
    spread(b)
    b = dev(p - 1, q)
    arrived(b, None)
    send(b, xall.at[b], 0, dev(p + 1, q))
    spread(b)
    b = dev(p + 2, q)
    arrived(b, 0)
    arrived(b, 1)
    spread(b)

    def member(g, i):
        if g == 0:
            return _near(i), 0
        if g == 3:
            return _near(i), 2
        return _near(2 * (g - 1) + i // 2), 1 + 2 * (i % 2)

    def source(g, i, own):
        dp, dq = member(g, i)
        if own:
            return dev(p + dp, q + dq)
        return _chip(o, q + dp, p + dq) * 2 + o

    rows = lax.broadcasted_iota(jnp.int32, (r, t), 0)
    nf = f // 3
    dt = d // 4

    def compute(g):
        for i in range(4):
            src = source(g, i, True)
            ref = x_ref if (g == 0 and i == 0) else xall.at[src]
            pltpu.make_async_copy(ref, xb.at[i], bsem.at[i]).start()
        for i in range(4):
            src = source(g, i, False)
            arrived(src, None)
            pltpu.make_async_copy(xall.at[src], xb.at[4 + i], bsem.at[4 + i]).start()

        def select(own):
            def body(i, carry):
                slot = i if own else 4 + i
                pltpu.make_async_copy(x_ref, xb.at[slot], bsem.at[slot]).wait()
                src = source(g, i, own)
                code = meta_ref[src].astype(jnp.int32) - me * r
                sel = jnp.zeros((r, t), F32)
                for j in range(8):
                    sel = sel + jnp.where(rows == code[j:j + 1, :], 1.0, 0.0)
                xs = jnp.dot(sel.astype(BF16), xb[slot], preferred_element_type=F32).astype(BF16)
                xg[:, pl.ds(slot * cap, cap), :] = xs.reshape(el, cap, d)
                return carry
            lax.fori_loop(0, 4, body, 0)
        select(True)
        select(False)
        if g == 0:
            for cp in loads:
                cp.wait()

        def expert(e, carry):
            def up(m, carry):
                cols = pl.ds(pl.multiple_of(m * nf, nf), nf)
                a = jnp.dot(xg[e], w1v[e, :, cols], preferred_element_type=F32)
                b = jnp.dot(xg[e], w3v[e, :, cols], preferred_element_type=F32)
                uv[:, cols] = (a * jax.nn.sigmoid(a) * b).astype(BF16)
                return carry
            lax.fori_loop(0, 3, up, 0)
            slot = e % 2

            def flush():
                for i in range(8):
                    pltpu.make_async_copy(hb.at[slot, pl.ds(i * cap, cap)], h_ref.at[0, pl.ds(0, cap)],
                                          osem.at[slot, i]).wait()
            if g > 0:
                flush()
            else:
                pl.when(e >= 2)(flush)

            def down(m, carry):
                cols = pl.ds(pl.multiple_of(m * dt, dt), dt)
                hb[slot, :, cols] = jnp.dot(uv[...], w2v[e, :, cols], preferred_element_type=F32).astype(BF16)
                return carry
            lax.fori_loop(0, 4, down, 0)
            for i in range(8):
                src = source(g, i % 4, i < 4)
                pltpu.make_async_copy(hb.at[slot, pl.ds(i * cap, cap)], h_ref.at[src, pl.ds(e * cap, cap)],
                                      osem.at[slot, i]).start()
            return carry
        lax.fori_loop(0, el, expert, 0)

    compute(0)
    for g in (1, 2):
        for i in range(4):
            b = source(g, i, True)
            arrived(b, None)
            if i % 2 == 0:
                send(b, xall.at[b], 1, dev(p, q - 1))
            else:
                send(b, xall.at[b], 0, dev(p, q + 1))
            send(b, xall.at[b], None, partner)
        compute(g)
    for i in range(4):
        b = source(3, i, True)
        arrived(b, 0)
        arrived(b, 1)
        send(b, xall.at[b], None, partner)
    compute(3)
    for slot in range(2):
        for i in range(8):
            pltpu.make_async_copy(hb.at[slot, pl.ds(i * cap, cap)], h_ref.at[0, pl.ds(0, cap)],
                                  osem.at[slot, i]).wait()
    for cp in sends:
        cp.wait_send()


def _return_kernel(n, r, h_ref, meta_ref, y_ref, rx, fwd, acc, r2, r1, gs, ssem, xsem, fsem, sem2, sem1):
    t, d = y_ref.shape
    me, c, cx, cy = _where(n)
    partner = me + 1 - 2 * c
    hr = r // 2
    ht = t // 2
    offs = (2, 1, 3, 0)
    greet = [partner]
    for k in (0, 1):
        pk, qk = (cx, cy) if k == 0 else (cy, cx)
        for s in (1, -1):
            for core in (0, 1):
                greet.append(_chip(k, pk, qk + s) * 2 + core)
    _greet(greet)
    sends = []

    def rcopy(src, dst, sem, to):
        cp = pltpu.make_async_remote_copy(src_ref=src, dst_ref=dst, send_sem=ssem.at[len(sends)], recv_sem=sem,
                                          device_id={'expert': to}, device_id_type=MESH)
        cp.start()
        sends.append(cp)

    def frame(k):
        return (cx, cy) if k == 0 else (cy, cx)

    def give(j):
        for k in (0, 1):
            pk, qk = frame(k)

            def rows(dq):
                return h_ref.at[_chip(k, pk + offs[j], qk + dq) * 2 + k]
            for s, dirn in ((1, 0), (-1, 1)):
                rcopy(rows(2).at[pl.ds(dirn * hr, hr)], fwd.at[k, dirn, j], fsem.at[k, dirn, j],
                      _chip(k, pk, qk + s) * 2 + c)
            for s, slot in ((1, 3), (-1, 1)):
                rcopy(rows(s), rx.at[j, slot, c], xsem.at[j, slot, c, 0], _chip(k, pk, qk + s) * 2 + k)
            far = pltpu.make_async_remote_copy(
                src_ref=rows(0), dst_ref=rx.at[j, 0, c], send_sem=ssem.at[len(sends)], recv_sem=xsem.at[j, 0, c, 0],
                device_id={'expert': partner}, device_id_type=MESH)
            here = pltpu.make_async_copy(rows(0), rx.at[j, 0, c], xsem.at[j, 0, c, 0])
            pl.when(c == k)(lambda: here.start())
            pl.when(c != k)(lambda: far.start())
            sends.append((k, far))

    def relay(j):
        for k in (0, 1):
            pk, qk = frame(k)
            for dirn, s in ((0, 1), (1, -1)):
                buf = fwd.at[k, dirn, j]
                pltpu.make_async_remote_copy(src_ref=buf, dst_ref=buf, send_sem=ssem.at[0],
                                             recv_sem=fsem.at[k, dirn, j], device_id={'expert': partner},
                                             device_id_type=MESH).wait_recv()
                rcopy(buf, rx.at[j, 2, c, pl.ds(dirn * hr, hr)], xsem.at[j, 2, c, dirn],
                      _chip(k, pk, qk + s) * 2 + k)

    o = 1 - c
    p = o * cx + c * cy
    q = o * cy + c * cx

    def collect(j):
        for slot in range(4):
            for core in (0, 1):
                if slot == 2:
                    for half in (0, 1):
                        pltpu.make_async_copy(h_ref.at[0, pl.ds(0, hr)], rx.at[j, slot, core, pl.ds(half * hr, hr)],
                                              xsem.at[j, slot, core, half]).wait()
                else:
                    pltpu.make_async_copy(h_ref.at[0], rx.at[j, slot, core], xsem.at[j, slot, core, 0]).wait()
        src = _chip(c, p + offs[j], q) * 2 + c
        meta = meta_ref[src].T
        lanes = lax.broadcasted_iota(jnp.int32, (t, r), 1)
        code = meta[:, :8].astype(jnp.int32)
        for slot in range(4):
            for core in (0, 1):
                base = (_chip(c, p, q + slot) * 2 + core) * r
                gm = jnp.zeros((t, r), F32)
                for i in range(8):
                    gm = gm + jnp.where(code[:, i:i + 1] - base == lanes, meta[:, 8 + i:9 + i], 0.0)
                hi = gm.astype(BF16)
                rest = gm - hi.astype(F32)
                mid = rest.astype(BF16)
                low = (rest - mid.astype(F32)).astype(BF16)
                cols = pl.ds((slot * 2 + core) * r, r)
                gs[0, :, cols] = hi
                gs[1, :, cols] = mid
                gs[2, :, cols] = low
        dt = d // 4

        def tile(m, carry):
            cols = pl.ds(pl.multiple_of(m * dt, dt), dt)
            rhs = rx[j, :, :, :, cols].reshape(8 * r, dt)
            s = jnp.dot(gs[0], rhs, preferred_element_type=F32)
            s = s + jnp.dot(gs[1], rhs, preferred_element_type=F32)
            s = s + jnp.dot(gs[2], rhs, preferred_element_type=F32)
            acc[j, :, cols] = s
            return carry
        lax.fori_loop(0, 4, tile, 0)

    def wait2(i):
        pltpu.make_async_remote_copy(src_ref=r2.at[i], dst_ref=r2.at[i], send_sem=ssem.at[0], recv_sem=sem2.at[i],
                                     device_id={'expert': partner}, device_id_type=MESH).wait_recv()

    def wait1(i):
        pltpu.make_async_remote_copy(src_ref=r1.at[i], dst_ref=r1.at[i], send_sem=ssem.at[0], recv_sem=sem1.at[i],
                                     device_id={'expert': partner}, device_id_type=MESH).wait_recv()

    up = _chip(c, p + 1, q) * 2 + c
    down = _chip(c, p - 1, q) * 2 + c
    give(0)
    give(1)
    relay(0)
    give(2)
    collect(0)
    rcopy(acc.at[0, pl.ds(0, ht)], r2.at[0], sem2.at[0], up)
    rcopy(acc.at[0, pl.ds(ht, ht)], r2.at[1], sem2.at[1], down)
    relay(1)
    give(3)
    collect(1)
    wait2(0)
    acc[1, 0:ht] = acc[1, 0:ht] + r2[0]
    rcopy(acc.at[1], r1.at[0], sem1.at[0], up)
    relay(2)
    collect(2)
    wait2(1)
    acc[2, ht:t] = acc[2, ht:t] + r2[1]
    rcopy(acc.at[2], r1.at[1], sem1.at[1], down)
    relay(3)
    collect(3)
    wait1(0)
    wait1(1)
    y_ref[...] = (acc[3] + r1[0] + r1[1]).astype(BF16)
    for cp in sends:
        if isinstance(cp, tuple):
            k, far = cp
            pl.when(c != k)(lambda: far.wait_send())
        else:
            cp.wait_send()


def solution(mesh):
    n = mesh.shape['expert']
    assert n == 2 * ND * ND

    def local(x, idx, g, hot_tok, w1, w3, w2):
        t, d = x.shape
        k = idx.shape[1]
        el, _, f = w1.shape
        e = el * n
        ch = hot_tok.shape[0]
        cap = max(ch, 2 * ((t * k - ch + e - 2) // (e - 1)))
        r = el * cap

        hit = idx[:, :, None] == jnp.arange(e, dtype=jnp.int32)
        chosen = hit.any(axis=1).astype(BF16)
        earlier = (jnp.arange(t)[:, None] > jnp.arange(t)[None, :]).astype(BF16)
        before = jnp.dot(earlier, chosen, preferred_element_type=F32)
        rank = jnp.where(hit, before[:, None, :], 0.0).sum(axis=2)
        code = (idx * cap).astype(F32) + rank
        meta = jnp.concatenate([code.T, g.T], axis=0)
        meta = lax.all_gather(meta, 'expert')

        anyspec = pl.BlockSpec(memory_space=pl.ANY)
        vspec = pl.BlockSpec(memory_space=pltpu.VMEM)
        h, _ = pl.pallas_call(
            functools.partial(_dispatch_kernel, n, el, cap),
            out_shape=[jax.ShapeDtypeStruct((n, r, d), BF16), jax.ShapeDtypeStruct((n, t, d), BF16)],
            in_specs=[anyspec, vspec, anyspec, anyspec, anyspec],
            out_specs=[anyspec, anyspec],
            scratch_shapes=[
                pltpu.VMEM(w1.shape, BF16), pltpu.VMEM(w3.shape, BF16), pltpu.VMEM(w2.shape, BF16),
                pltpu.VMEM((8, t, d), BF16), pltpu.VMEM((el, 8 * cap, d), BF16),
                pltpu.VMEM((8 * cap, f), BF16), pltpu.VMEM((2, 8 * cap, d), BF16),
                pltpu.SemaphoreType.DMA((3,)), pltpu.SemaphoreType.DMA((8,)), pltpu.SemaphoreType.DMA((2, 8)),
                pltpu.SemaphoreType.DMA((36,)), pltpu.SemaphoreType.DMA((n, 2)),
            ],
            compiler_params=pltpu.CompilerParams(collective_id=0, has_side_effects=True,
                                                 vmem_limit_bytes=66_000_000),
        )(x, meta, w1, w3, w2)
        return pl.pallas_call(
            functools.partial(_return_kernel, n, r),
            out_shape=jax.ShapeDtypeStruct((t, d), BF16),
            in_specs=[anyspec, vspec],
            out_specs=vspec,
            scratch_shapes=[
                pltpu.VMEM((4, 4, 2, r, d), BF16), pltpu.VMEM((2, 2, 4, r // 2, d), BF16),
                pltpu.VMEM((4, t, d), F32), pltpu.VMEM((2, t // 2, d), F32), pltpu.VMEM((2, t, d), F32),
                pltpu.VMEM((3, t, 8 * r), BF16),
                pltpu.SemaphoreType.DMA((60,)), pltpu.SemaphoreType.DMA((4, 4, 2, 2)),
                pltpu.SemaphoreType.DMA((2, 2, 4)), pltpu.SemaphoreType.DMA((2,)), pltpu.SemaphoreType.DMA((2,)),
            ],
            compiler_params=pltpu.CompilerParams(collective_id=1, has_side_effects=True,
                                                 vmem_limit_bytes=60_000_000),
        )(h, meta)

    rows = P(('data', 'expert'))
    wspec = P('expert')
    return jax.shard_map(local, mesh=mesh, in_specs=(rows, rows, rows, rows, wspec, wspec, wspec), out_specs=rows,
                         check_vma=False)
```

```python
import functools
import math

import jax
import jax.numpy as jnp
from jax import lax
from jax.experimental import pallas as pl
from jax.experimental.pallas import tpu as pltpu
from jax.sharding import PartitionSpec as P

MESH = pl.DeviceIdType.MESH
F32 = jnp.float32
BF16 = jnp.bfloat16
ND = 4


def _where(n):
    me = lax.axis_index('expert')
    c = me % 2
    chip = me // 2
    return me, c, chip % ND, chip // ND


def _chip(k, p, q):
    p = p % ND
    q = q % ND
    return (1 - k) * (q * ND + p) + k * (p * ND + q)


def _near(j):
    return j + j // 2 - 2 * (j // 3)


def _greet(devs):
    bar = pltpu.get_barrier_semaphore()
    for dev in devs:
        pl.semaphore_signal(bar, inc=1, device_id={'expert': dev}, device_id_type=MESH)
    pl.semaphore_wait(bar, len(devs))


def _dispatch_kernel(n, el, cap, x_ref, meta_ref, w1_ref, w3_ref, w2_ref, h_ref, xall, metas,
                     w1v, w3v, w2v, xb, xg, uv, hb, wsem, bsem, osem, ssem, rsem, msem, mrsem):
    t, d = x_ref.shape
    f = w1v.shape[2]
    r = el * cap
    ht = t // 2
    me, c, cx, cy = _where(n)
    o = 1 - c
    p = o * cx + c * cy
    q = o * cy + c * cx
    partner = me + 1 - 2 * c

    def dev(pp, qq):
        return _chip(c, pp, qq) * 2 + c

    pu, pd, qu, qd = dev(p + 1, q), dev(p + 3, q), dev(p, q + 1), dev(p, q + 3)
    _greet([pu, pd, qu, qd, partner])

    loads = []
    for i, (a, b) in enumerate(((w1_ref, w1v), (w3_ref, w3v), (w2_ref, w2v))):
        loads.append(pltpu.make_async_copy(a, b, wsem.at[i]))
    count = [0, 0]

    def bump(i):
        count[i] += 1
        return count[i] - 1

    def copy(b, ref, half, to, sem):
        rows = pl.ds(half * ht, ht)
        return pltpu.make_async_remote_copy(
            src_ref=ref.at[rows], dst_ref=xall.at[b, rows], send_sem=ssem.at[sem], recv_sem=rsem.at[b, half],
            device_id={'expert': to}, device_id_type=MESH)

    def note(b, ref, to, sem):
        return pltpu.make_async_remote_copy(
            src_ref=ref, dst_ref=metas.at[b], send_sem=msem.at[sem], recv_sem=mrsem.at[b],
            device_id={'expert': to}, device_id_type=MESH)

    def send(b, ref, half, to):
        copy(b, ref, half, to, bump(0)).start()

    def tell(b, ref, to):
        note(b, ref, to, bump(1)).start()

    def arrived(b, half):
        copy(b, xall.at[b], half, partner, 0).wait_recv()

    def told(b):
        note(b, metas.at[b], partner, 0).wait_recv()

    for k in (0, 1):
        send(me, x_ref, k, pu)
        send(me, x_ref, 1 - k, pd)
        send(me, x_ref, k, qu)
        send(me, x_ref, 1 - k, qd)
        if k == 0:
            for to in (pu, pd, qu, qd, partner):
                tell(me, meta_ref, to)
    for k in (0, 1):
        send(me, x_ref, k, partner)
    for cp in loads:
        cp.start()
    metas[me] = meta_ref[...]

    def spread(b, half):
        for to in (qu, qd, partner):
            send(b, xall.at[b], half, to)

    def announce(b, first):
        told(b)
        for to in first + (qu, qd, partner):
            tell(b, metas.at[b], to)

    arrived(pd, 0)
    send(pd, xall.at[pd], 0, pu)
    spread(pd, 0)
    arrived(pu, 1)
    send(pu, xall.at[pu], 1, pd)
    spread(pu, 1)
    announce(pd, (pu,))
    announce(pu, ())
    arrived(pd, 1)
    spread(pd, 1)
    arrived(pu, 0)
    spread(pu, 0)
    far = dev(p + 2, q)
    arrived(far, 0)
    spread(far, 0)
    announce(far, ())
    arrived(far, 1)
    spread(far, 1)
    base, mbase = count

    def member(g, i):
        z = ((g + 1) // 2) % 2
        dp = _near(z * (2 * g - 2 + i // 2) + (1 - z) * i)
        dq = z * (1 + 2 * (i % 2)) + (1 - z) * 2 * (g // 3)
        return dp, dq

    def spot(g, i, own):
        dp, dq = member(g, i)
        if own:
            return c, (p + dp) % ND, (q + dq) % ND
        return o, (q + dp) % ND, (p + dq) % ND

    def source(g, i, own):
        k, pp, qq = spot(g, i, own)
        return _chip(k, pp, qq) * 2 + k

    rows = lax.broadcasted_iota(jnp.int32, (r, t), 0)
    nf = f // 3
    dt = d // 4

    def flush(slot):
        for i in range(8):
            pltpu.make_async_copy(hb.at[slot, pl.ds(i * cap, cap)], h_ref.at[0, 0, 0, pl.ds(0, cap)],
                                  osem.at[slot, i]).wait()

    def pass_on(g):
        for i in range(4):
            b = source(g, i, True)
            first = 1 - i % 2
            at = base + ((g - 1) * 4 + i) * 3
            arrived(b, first)
            copy(b, xall.at[b], first, (qd, qu)[i % 2], at).start()
            copy(b, xall.at[b], first, partner, at + 1).start()
            arrived(b, 1 - first)
            copy(b, xall.at[b], 1 - first, partner, at + 2).start()
            told(b)
            mat = mbase + ((g - 1) * 4 + i) * 2
            note(b, metas.at[b], partner, mat).start()
            if i % 2 == 1:
                note(b, metas.at[b], qu, mat + 1).start()

    def finish(g):
        for i in range(4):
            b = source(g, i, True)
            at = base + 24 + i * 2
            arrived(b, 0)
            copy(b, xall.at[b], 0, partner, at).start()
            told(b)
            note(b, metas.at[b], partner, mbase + 16 + i).start()
            arrived(b, 1)
            copy(b, xall.at[b], 1, partner, at + 1).start()

    def group(g, carry):
        pl.when(((g + 1) // 2) % 2 == 1)(lambda: pass_on(g))
        pl.when(g == 3)(lambda: finish(g))
        for i in range(4):
            src = source(g, i, True)
            fetch = pltpu.make_async_copy(xall.at[src], xb.at[i], bsem.at[i])
            if i == 0:
                pl.when(g > 0)(fetch.start)
                pl.when(g == 0)(pltpu.make_async_copy(x_ref, xb.at[0], bsem.at[0]).start)
            else:
                fetch.start()
        for i in range(4):
            src = source(g, i, False)
            arrived(src, 0)
            arrived(src, 1)
            told(src)
            pltpu.make_async_copy(xall.at[src], xb.at[4 + i], bsem.at[4 + i]).start()
        for slot in range(8):
            code = metas[source(g, slot % 4, slot < 4)].astype(jnp.int32) - me * r
            sel = jnp.zeros((r, t), F32)
            for j in range(8):
                sel = sel + jnp.where(rows == code[j:j + 1, :], 1.0, 0.0)
            pltpu.make_async_copy(x_ref, xb.at[slot], bsem.at[slot]).wait()
            xs = jnp.dot(sel.astype(BF16), xb[slot], preferred_element_type=F32).astype(BF16)
            xg[:, slot * cap:(slot + 1) * cap, :] = xs.reshape(el, cap, d)

        def ready():
            for cp in loads:
                cp.wait()
        pl.when(g == 0)(ready)

        def expert(e, carry):
            for m in range(3):
                cols = slice(m * nf, (m + 1) * nf)
                a = jnp.dot(xg[e], w1v[e, :, cols], preferred_element_type=F32)
                b = jnp.dot(xg[e], w3v[e, :, cols], preferred_element_type=F32)
                uv[:, cols] = (a * jax.nn.sigmoid(a) * b).astype(BF16)
            slot = e % 2
            pl.when(g * el + e >= 2)(lambda: flush(slot))
            for m in range(4):
                cols = slice(m * dt, (m + 1) * dt)
                hb[slot, :, cols] = jnp.dot(uv[...], w2v[e, :, cols], preferred_element_type=F32).astype(BF16)
            for i in range(8):
                k, pp, qq = spot(g, i % 4, i < 4)
                pltpu.make_async_copy(hb.at[slot, pl.ds(i * cap, cap)], h_ref.at[k, qq, pp, pl.ds(e * cap, cap)],
                                      osem.at[slot, i]).start()
            return carry
        return lax.fori_loop(0, el, expert, carry)

    lax.fori_loop(0, 4, group, 0)
    flush(0)
    flush(1)

    def sent(i, carry):
        copy(me, x_ref, 0, partner, i).wait_send()
        return carry
    lax.fori_loop(0, base + 32, sent, 0)

    def noted(i, carry):
        note(me, meta_ref, partner, i).wait_send()
        return carry
    lax.fori_loop(0, mbase, noted, 0)
    for i in range(8):
        note(me, meta_ref, partner, mbase + 2 * i).wait_send()
        if i % 2 == 1:
            note(me, meta_ref, partner, mbase + 2 * i + 1).wait_send()
    for i in range(4):
        note(me, meta_ref, partner, mbase + 16 + i).wait_send()


def _return_kernel(n, r, nc, h_ref, meta_ref, y_ref, rx, fwd, acc, r2, r1, gs, gsem, lsem, psem, xsem, fsem,
                   sem2, sem1):
    t, d = y_ref.shape
    dc = d // nc
    me, c, cx, cy = _where(n)
    partner = me + 1 - 2 * c
    ht = t // 2
    frames = ((cx, cy), (cy, cx))
    greet = [partner]
    for k in (0, 1):
        pk, qk = frames[k]
        for s in (1, 3):
            for core in (0, 1):
                greet.append(_chip(k, pk, qk + s) * 2 + core)
    _greet(greet)
    o = 1 - c
    p = o * cx + c * cy
    q = o * cy + c * cx

    def columns(ci):
        return pl.ds(pl.multiple_of(ci * dc, dc), dc)

    def rcopy(src, dst, ssem, rsem, to):
        return pltpu.make_async_remote_copy(src_ref=src, dst_ref=dst, send_sem=ssem, recv_sem=rsem,
                                            device_id={'expert': to}, device_id_type=MESH)

    def rows(k, dq, ci):
        return h_ref.at[k, (frames[k][1] + dq) % ND, :, :, columns(ci)]

    def far(k, dirn, ci):
        pk, qk = frames[k]
        src = h_ref.at[k, (qk + 2) % ND, pl.ds(dirn * 2, 2), :, columns(ci)]
        return rcopy(src, fwd.at[ci, k, dirn], gsem.at[ci, k, dirn], fsem.at[ci, k, dirn],
                     _chip(k, pk, qk + 1 + 2 * dirn) * 2 + c)

    def near(k, dirn, ci):
        pk, qk = frames[k]
        slot = 3 - 2 * dirn
        return rcopy(rows(k, 1 + 2 * dirn, ci), rx.at[ci, slot, c], gsem.at[ci, k, 2 + dirn],
                     xsem.at[ci, slot, c, 0], _chip(k, pk, qk + 1 + 2 * dirn) * 2 + k)

    def other(k, ci):
        return rcopy(rows(k, 0, ci), rx.at[ci, 0, c], gsem.at[ci, k, 4], xsem.at[ci, 0, c, 0], partner)

    def hop(k, dirn, ci):
        pk, qk = frames[k]
        return rcopy(fwd.at[ci, k, dirn], rx.at[ci, 2, c, pl.ds(dirn * 2, 2)], lsem.at[ci, k, dirn],
                     xsem.at[ci, 2, c, dirn], _chip(k, pk, qk + 1 + 2 * dirn) * 2 + k)

    def give(ci):
        for k in (0, 1):
            far(k, 0, ci).start()
            far(k, 1, ci).start()
        for k in (0, 1):
            near(k, 0, ci).start()
            near(k, 1, ci).start()
        for k in (0, 1):
            pl.when(c == k)(pltpu.make_async_copy(rows(k, 0, ci), rx.at[ci, 0, c], xsem.at[ci, 0, c, 0]).start)
            pl.when(c != k)(other(k, ci).start)

    def relay(ci):
        for k in (0, 1):
            for dirn in (0, 1):
                far(k, dirn, ci).wait_recv()
                hop(k, dirn, ci).start()

    def collect(ci):
        for slot in range(4):
            for core in (0, 1):
                if slot == 2:
                    for half in (0, 1):
                        two = pl.ds(half * 2, 2)
                        pltpu.make_async_copy(h_ref.at[0, 0, two, :, columns(0)], rx.at[ci, slot, core, two],
                                              xsem.at[ci, slot, core, half]).wait()
                else:
                    pltpu.make_async_copy(h_ref.at[0, 0, :, :, columns(0)], rx.at[ci, slot, core],
                                          xsem.at[ci, slot, core, 0]).wait()

    lanes = lax.broadcasted_iota(jnp.int32, (t, r), 1)

    def gates(pp, carry):
        src = _chip(c, pp, q) * 2 + c
        meta = meta_ref[src].T
        code = meta[:, :8].astype(jnp.int32)
        for slot in range(4):
            for core in (0, 1):
                base = (_chip(c, p, q + slot) * 2 + core) * r
                gm = jnp.zeros((t, r), F32)
                for i in range(8):
                    gm = gm + jnp.where(code[:, i:i + 1] - base == lanes, meta[:, 8 + i:9 + i], 0.0)
                hi = gm.astype(BF16)
                rest = gm - hi.astype(F32)
                mid = rest.astype(BF16)
                low = (rest - mid.astype(F32)).astype(BF16)
                cols = slice((slot * 2 + core) * r, (slot * 2 + core + 1) * r)
                gs[pp, 0, :, cols] = hi
                gs[pp, 1, :, cols] = mid
                gs[pp, 2, :, cols] = low
        return carry

    def weigh(ci, j, off):
        pp = (p + off) % ND
        rhs = rx[ci, :, :, pp].reshape(8 * r, dc)
        s = jnp.dot(gs[pp, 0], rhs, preferred_element_type=F32)
        s = s + jnp.dot(gs[pp, 1], rhs, preferred_element_type=F32)
        s = s + jnp.dot(gs[pp, 2], rhs, preferred_element_type=F32)
        acc[ci, j] = s

    ends = (_chip(c, p + 1, q) * 2 + c, _chip(c, p + 3, q) * 2 + c)

    def half(i, ci):
        return rcopy(acc.at[ci, 0, pl.ds(i * ht, ht)], r2.at[ci, i], psem.at[ci, i], sem2.at[ci, i], ends[i])

    def whole(i, ci):
        return rcopy(acc.at[ci, 1 + i], r1.at[ci, i], psem.at[ci, 2 + i], sem1.at[ci, i], ends[i])

    def finalize(ci):
        whole(0, ci).wait_recv()
        whole(1, ci).wait_recv()
        y_ref[:, columns(ci)] = (acc[ci, 3] + r1[ci, 0] + r1[ci, 1]).astype(BF16)

    def step(ci, carry):
        pl.when(ci + 1 < nc)(lambda: relay(ci + 1))
        pl.when(ci + 2 < nc)(lambda: give(ci + 2))
        collect(ci)
        weigh(ci, 0, 2)
        half(0, ci).start()
        half(1, ci).start()
        weigh(ci, 1, 1)
        weigh(ci, 2, 3)
        for i in (0, 1):
            half(i, ci).wait_recv()
            own = pl.ds(i * ht, ht)
            acc[ci, 1 + i, own] = acc[ci, 1 + i, own] + r2[ci, i]
            whole(i, ci).start()
        weigh(ci, 3, 0)
        pl.when(ci > 0)(lambda: finalize(ci - 1))
        return carry

    give(0)
    relay(0)
    give(1)
    lax.fori_loop(0, ND, gates, 0)
    lax.fori_loop(0, nc, step, 0)
    finalize(nc - 1)

    def drain(ci, carry):
        for k in (0, 1):
            for dirn in (0, 1):
                far(k, dirn, ci).wait_send()
                near(k, dirn, ci).wait_send()
                hop(k, dirn, ci).wait_send()
            pl.when(c != k)(other(k, ci).wait_send)
        for i in (0, 1):
            half(i, ci).wait_send()
            whole(i, ci).wait_send()
        return carry
    lax.fori_loop(0, nc, drain, 0)


def solution(mesh):
    n = mesh.shape['expert']
    assert n == 2 * ND * ND

    def local(x, idx, g, hot_tok, w1, w3, w2):
        t, d = x.shape
        k = idx.shape[1]
        el, _, f = w1.shape
        e = el * n
        ch = hot_tok.shape[0]
        cap = max(ch, 2 * ((t * k - ch + e - 2) // (e - 1)))
        r = el * cap
        nc = 4
        dc = d // nc

        hit = idx[:, :, None] == jnp.arange(e, dtype=jnp.int32)
        chosen = hit.any(axis=1).astype(BF16)
        earlier = (jnp.arange(t)[:, None] > jnp.arange(t)[None, :]).astype(BF16)
        before = jnp.dot(earlier, chosen, preferred_element_type=F32)
        rank = jnp.where(hit, before[:, None, :], 0.0).sum(axis=2)
        code = (idx * cap).astype(F32) + rank
        meta = jnp.concatenate([code.T, g.T], axis=0)

        anyspec = pl.BlockSpec(memory_space=pl.ANY)
        vspec = pl.BlockSpec(memory_space=pltpu.VMEM)
        h, _, metas = pl.pallas_call(
            functools.partial(_dispatch_kernel, n, el, cap),
            out_shape=[jax.ShapeDtypeStruct((2, ND, ND, r, d), BF16), jax.ShapeDtypeStruct((n, t, d), BF16),
                       jax.ShapeDtypeStruct((n,) + meta.shape, F32)],
            in_specs=[anyspec, vspec, anyspec, anyspec, anyspec],
            out_specs=[anyspec, anyspec, vspec],
            scratch_shapes=[
                pltpu.VMEM(w1.shape, BF16), pltpu.VMEM(w3.shape, BF16), pltpu.VMEM(w2.shape, BF16),
                pltpu.VMEM((8, t, d), BF16), pltpu.VMEM((el, 8 * cap, d), BF16),
                pltpu.VMEM((8 * cap, f), BF16), pltpu.VMEM((2, 8 * cap, d), BF16),
                pltpu.SemaphoreType.DMA((3,)), pltpu.SemaphoreType.DMA((8,)), pltpu.SemaphoreType.DMA((2, 8)),
                pltpu.SemaphoreType.DMA((62,)), pltpu.SemaphoreType.DMA((n, 2)),
                pltpu.SemaphoreType.DMA((35,)), pltpu.SemaphoreType.DMA((n,)),
            ],
            compiler_params=pltpu.CompilerParams(collective_id=0, has_side_effects=True,
                                                 vmem_limit_bytes=66_000_000),
        )(x, meta, w1, w3, w2)
        return pl.pallas_call(
            functools.partial(_return_kernel, n, r, nc),
            out_shape=jax.ShapeDtypeStruct((t, d), BF16),
            in_specs=[anyspec, vspec],
            out_specs=vspec,
            scratch_shapes=[
                pltpu.VMEM((nc, 4, 2, ND, r, dc), BF16), pltpu.VMEM((nc, 2, 2, 2, r, dc), BF16),
                pltpu.VMEM((nc, 4, t, dc), F32), pltpu.VMEM((nc, 2, t // 2, dc), F32),
                pltpu.VMEM((nc, 2, t, dc), F32), pltpu.VMEM((ND, 3, t, 8 * r), BF16),
                pltpu.SemaphoreType.DMA((nc, 2, 5)), pltpu.SemaphoreType.DMA((nc, 2, 2)),
                pltpu.SemaphoreType.DMA((nc, 4)), pltpu.SemaphoreType.DMA((nc, 4, 2, 2)),
                pltpu.SemaphoreType.DMA((nc, 2, 2)), pltpu.SemaphoreType.DMA((nc, 2)),
                pltpu.SemaphoreType.DMA((nc, 2)),
            ],
            compiler_params=pltpu.CompilerParams(collective_id=1, has_side_effects=True,
                                                 vmem_limit_bytes=60_000_000),
        )(h, metas)

    rows = P(('data', 'expert'))
    wspec = P('expert')
    return jax.shard_map(local, mesh=mesh, in_specs=(rows, rows, rows, rows, wspec, wspec, wspec), out_specs=rows,
                         check_vma=False)
```

```python
import functools
import math

import jax
import jax.numpy as jnp
from jax import lax
from jax.experimental import pallas as pl
from jax.experimental.pallas import tpu as pltpu
from jax.sharding import PartitionSpec as P

MESH = pl.DeviceIdType.MESH
F32 = jnp.float32
BF16 = jnp.bfloat16
ND = 4


def _where(n):
    me = lax.axis_index('expert')
    c = me % 2
    chip = me // 2
    return me, c, chip % ND, chip // ND


def _chip(k, p, q):
    p = p % ND
    q = q % ND
    return (1 - k) * (q * ND + p) + k * (p * ND + q)


def _around(frames):
    return [_chip(k, frames[k][0], frames[k][1] + s) * 2 + core for k in (0, 1) for s in (1, 3) for core in (0, 1)]


def _greet(devs):
    bar = pltpu.get_barrier_semaphore()
    for dev in devs:
        pl.semaphore_signal(bar, inc=1, device_id={'expert': dev}, device_id_type=MESH)
    pl.semaphore_wait(bar, len(devs))


def _dispatch_kernel(n, el, cap, nc, x_ref, meta_ref, w1_ref, w3_ref, w2_ref, *refs):
    h_refs, (xall, metas, rn), refs = refs[:nc], refs[nc:nc + 3], refs[nc + 3:]
    hbs, (w1v, w3v, w2v, xb, xg, uv, wsem, bsem, osem, ssem, rsem, msem, mrsem,
          nsem, nrsem) = refs[:nc], refs[nc:]
    t, d = x_ref.shape
    f = w1v.shape[2]
    r = el * cap
    ht = t // 2
    me, c, cx, cy = _where(n)
    o = 1 - c
    p = o * cx + c * cy
    q = o * cy + c * cx
    partner = me + 1 - 2 * c

    def dev(pp, qq):
        return _chip(c, pp, qq) * 2 + c

    pu, pd, qu, qd = dev(p + 1, q), dev(p + 3, q), dev(p, q + 1), dev(p, q + 3)
    frames = ((cx, cy), (cy, cx))
    _greet(_around(frames) + [partner])

    loads = []
    for i, (a, b) in enumerate(((w1_ref, w1v), (w3_ref, w3v), (w2_ref, w2v))):
        loads.append(pltpu.make_async_copy(a, b, wsem.at[i]))
    count = [0, 0]

    def bump(i):
        count[i] += 1
        return count[i] - 1

    def copy(b, ref, half, to, sem):
        rows = pl.ds(0, t) if half is None else pl.ds(half * ht, ht)
        half = half or 0
        return pltpu.make_async_remote_copy(
            src_ref=ref.at[rows], dst_ref=xall.at[b, rows], send_sem=ssem.at[sem], recv_sem=rsem.at[b, half],
            device_id={'expert': to}, device_id_type=MESH)

    def note(b, ref, to, sem):
        return pltpu.make_async_remote_copy(
            src_ref=ref, dst_ref=metas.at[b], send_sem=msem.at[sem], recv_sem=mrsem.at[b],
            device_id={'expert': to}, device_id_type=MESH)

    sizes = []

    def send(b, ref, half, to):
        sizes.append(half)
        copy(b, ref, half, to, bump(0)).start()

    def tell(b, ref, to):
        note(b, ref, to, bump(1)).start()

    def arrived(b, half):
        copy(b, xall.at[b], half, partner, 0).wait_recv()

    def told(b):
        note(b, metas.at[b], partner, 0).wait_recv()

    for k in (0, 1):
        send(me, x_ref, k, pu)
        send(me, x_ref, 1 - k, pd)
        send(me, x_ref, k, qu)
        send(me, x_ref, 1 - k, qd)
        if k == 0:
            for to in (pu, pd, qu, qd, partner):
                tell(me, meta_ref, to)
    send(me, x_ref, None, partner)
    for cp in loads:
        cp.start()
    metas[me] = meta_ref[...]

    def spread(b):
        for to in (qu, qd, partner):
            send(b, xall.at[b], None, to)

    def announce(b, *to):
        told(b)
        for to in to:
            tell(b, metas.at[b], to)

    def ring():
        arrived(pd, 0)
        send(pd, xall.at[pd], 0, pu)
        arrived(pu, 1)
        send(pu, xall.at[pu], 1, pd)
        announce(pd, pu, qu, qd, partner)
        announce(pu, qu, qd, partner)
        arrived(pd, 1)
        spread(pd)
        arrived(pu, 0)
        spread(pu)

    def take(dp, dq):
        b = dev(p + dp, q + dq)
        first = 1 if dq == 1 else 0
        on = qd if dq == 1 else qu
        if dq in (1, 3) and dp:
            arrived(b, None)
            send(b, xall.at[b], first, on)
        else:
            arrived(b, first)
            if dq in (1, 3):
                send(b, xall.at[b], first, on)
            arrived(b, 1 - first)
        if dq == 0:
            spread(b)
            announce(b, qu, qd, partner)
            return
        send(b, xall.at[b], None, partner)
        if dq == 3:
            announce(b, qu, partner)
        else:
            announce(b, partner)

    def spot(dp, dq, own):
        if own:
            return c, (p + dp) % ND, (q + dq) % ND
        return o, (q + dp) % ND, (p + dq) % ND

    def source(dp, dq, own):
        k, pp, qq = spot(dp, dq, own)
        return _chip(k, pp, qq) * 2 + k

    rows = lax.broadcasted_iota(jnp.int32, (r, t), 0)
    nf = f // 3
    dt = math.gcd(512, *(hb.shape[-1] for hb in hbs))

    def flush(slot, m):
        for i in range(m):
            for j in range(nc):
                pltpu.make_async_copy(hbs[j].at[slot, pl.ds(i * cap, cap)], h_refs[j].at[0, 0, 0, pl.ds(0, cap)],
                                      osem.at[slot, i, j]).wait()

    def fetch(slot, dp, dq, own):
        src = source(dp, dq, own)
        ref = x_ref if own and dp == 0 and dq == 0 else xall.at[src]
        pltpu.make_async_copy(ref, xb.at[slot], bsem.at[slot]).start()

    def select(slot, dp, dq, own):
        code = metas[source(dp, dq, own)].astype(jnp.int32) - me * r
        hit = rows == code[0:1, :]
        for j in range(1, 8):
            hit = hit | (rows == code[j:j + 1, :])
        sel = jnp.where(hit, 1.0, 0.0).astype(BF16)
        pltpu.make_async_copy(x_ref, xb.at[slot], bsem.at[slot]).wait()
        xs = jnp.dot(sel, xb[slot], preferred_element_type=F32).astype(BF16)
        xg[:, slot * cap:(slot + 1) * cap, :] = xs.reshape(el, cap, d)

    def group(members, before, first=False):
        nb = len(members)
        m = 2 * nb * cap
        for i, (dp, dq) in enumerate(members):
            fetch(i, dp, dq, True)
        for i, (dp, dq) in enumerate(members):
            select(i, dp, dq, True)
        for i, (dp, dq) in enumerate(members):
            src = source(dp, dq, False)
            arrived(src, None)
            told(src)
            fetch(nb + i, dp, dq, False)
        for i, (dp, dq) in enumerate(members):
            select(nb + i, dp, dq, False)
        if first:
            for cp in loads:
                cp.wait()

        def expert(e, carry):
            for i in range(3):
                cols = slice(i * nf, (i + 1) * nf)
                a = jnp.dot(xg[e, 0:m], w1v[e, :, cols], preferred_element_type=F32)
                b = jnp.dot(xg[e, 0:m], w3v[e, :, cols], preferred_element_type=F32)
                uv[0:m, cols] = (a * jax.nn.sigmoid(a) * b).astype(BF16)
            slot = e % 2
            if before == 2 * nb:
                flush(slot, before)
            else:
                pl.when(e >= 2)(lambda: flush(slot, 2 * nb))
                if before:
                    pl.when(e < 2)(lambda: flush(slot, before))
            at = 0
            for hb in hbs:
                for i in range(0, hb.shape[-1], dt):
                    hb[slot, 0:m, i:i + dt] = jnp.dot(uv[0:m], w2v[e, :, at:at + dt],
                                                      preferred_element_type=F32).astype(BF16)
                    at += dt
            for i in range(2 * nb):
                k, pp, qq = spot(*members[i % nb], i < nb)
                for j in range(nc):
                    pltpu.make_async_copy(hbs[j].at[slot, pl.ds(i * cap, cap)],
                                          h_refs[j].at[k, qq, pp, pl.ds(e * cap, cap)], osem.at[slot, i, j]).start()
            return carry
        lax.fori_loop(0, el, expert, 0)
        return 2 * nb

    ring()
    take(0, 1)
    take(0, 3)
    done = group(((0, 0), (1, 0), (3, 0), (0, 1)), 0, True)
    take(2, 0)
    take(3, 1)
    take(3, 3)
    done = group(((0, 3), (2, 0), (3, 1), (3, 3)), done)
    take(1, 1)
    take(1, 3)
    take(2, 1)
    take(2, 3)
    done = group(((1, 1), (1, 3), (2, 1), (2, 3)), done)
    flush(0, done)
    flush(1, done)
    ahead = []
    for k in (0, 1):
        pk, qk = frames[k]
        for dirn, s in ((0, 1), (1, 3)):
            ahead.append(pltpu.make_async_remote_copy(
                src_ref=h_refs[0].at[k, (qk + s) % ND], dst_ref=rn.at[dirn, c], send_sem=nsem.at[k, dirn],
                recv_sem=nrsem.at[dirn, c], device_id={'expert': _chip(k, pk, qk + s) * 2 + k}, device_id_type=MESH))
    for cp in ahead:
        cp.start()
    take(0, 2)
    take(3, 2)
    done = group(((0, 2), (3, 2)), 0)
    take(1, 2)
    take(2, 2)
    done = group(((1, 2), (2, 2)), done)
    flush(0, done)
    flush(1, done)

    for i, half in enumerate(sizes):
        copy(me, x_ref, half, partner, i).wait_send()

    for cp in ahead:
        cp.wait_send()
    for dirn in (0, 1):
        for core in (0, 1):
            pltpu.make_async_remote_copy(
                src_ref=rn.at[dirn, core], dst_ref=rn.at[dirn, core], send_sem=nsem.at[0, 0],
                recv_sem=nrsem.at[dirn, core], device_id={'expert': partner}, device_id_type=MESH).wait_recv()

    def noted(i, carry):
        note(me, meta_ref, partner, i).wait_send()
        return carry
    lax.fori_loop(0, count[1], noted, 0)
    assert count == [40, 31]


def _return_kernel(n, r, nc, *refs):
    h_refs, (meta_ref, rn, y_ref), refs = refs[:nc], refs[nc:nc + 3], refs[nc + 3:]
    rx, fwd, acc, r2, r1 = (refs[i * nc:(i + 1) * nc] for i in range(5))
    gs, gsem, lsem, psem, xsem, fsem, sem2, sem1 = refs[5 * nc:]
    t, d = y_ref.shape
    widths = [h.shape[-1] for h in h_refs]
    starts = [sum(widths[:i]) for i in range(nc)]
    me, c, cx, cy = _where(n)
    partner = me + 1 - 2 * c
    ht = t // 2
    frames = ((cx, cy), (cy, cx))
    _greet(_around(frames) + [partner])
    o = 1 - c
    p = o * cx + c * cy
    q = o * cy + c * cx

    def rcopy(src, dst, ssem, rsem, to):
        return pltpu.make_async_remote_copy(src_ref=src, dst_ref=dst, send_sem=ssem, recv_sem=rsem,
                                            device_id={'expert': to}, device_id_type=MESH)

    def rows(k, dq, ci):
        return h_refs[ci].at[k, (frames[k][1] + dq) % ND]

    def far(k, dirn, ci):
        pk, qk = frames[k]
        src = h_refs[ci].at[k, (qk + 2) % ND, pl.ds(dirn * 2, 2)]
        return rcopy(src, fwd[ci].at[k, dirn], gsem.at[ci, k, dirn], fsem.at[ci, k, dirn],
                     _chip(k, pk, qk + 1 + 2 * dirn) * 2 + c)

    def near(k, dirn, ci):
        pk, qk = frames[k]
        slot = 3 - 2 * dirn
        return rcopy(rows(k, 1 + 2 * dirn, ci), rx[ci].at[slot, c], gsem.at[ci, k, 2 + dirn],
                     xsem.at[ci, slot, c, 0], _chip(k, pk, qk + 1 + 2 * dirn) * 2 + k)

    def other(k, ci):
        return rcopy(rows(k, 0, ci), rx[ci].at[0, c], gsem.at[ci, k, 4], xsem.at[ci, 0, c, 0], partner)

    def hop(k, dirn, ci):
        pk, qk = frames[k]
        return rcopy(fwd[ci].at[k, dirn], rx[ci].at[2, c, pl.ds(dirn * 2, 2)], lsem.at[ci, k, dirn],
                     xsem.at[ci, 2, c, dirn], _chip(k, pk, qk + 1 + 2 * dirn) * 2 + k)

    def give(ci):
        for k in (0, 1):
            far(k, 0, ci).start()
            far(k, 1, ci).start()
        for k in (0, 1):
            for dirn in (0, 1):
                if ci:
                    near(k, dirn, ci).start()
                else:
                    slot = 3 - 2 * dirn
                    pltpu.make_async_copy(rn.at[dirn, k], rx[0].at[slot, k], xsem.at[0, slot, k, 0]).start()
        for k in (0, 1):
            pl.when(c == k)(pltpu.make_async_copy(rows(k, 0, ci), rx[ci].at[0, c], xsem.at[ci, 0, c, 0]).start)
            pl.when(c != k)(other(k, ci).start)

    def relay(ci):
        for k in (0, 1):
            for dirn in (0, 1):
                far(k, dirn, ci).wait_recv()
                hop(k, dirn, ci).start()

    def collect(ci):
        for slot in range(4):
            for core in (0, 1):
                if slot == 2:
                    for half in (0, 1):
                        two = pl.ds(half * 2, 2)
                        pltpu.make_async_copy(h_refs[ci].at[0, 0, two], rx[ci].at[slot, core, two],
                                              xsem.at[ci, slot, core, half]).wait()
                else:
                    pltpu.make_async_copy(h_refs[ci].at[0, 0], rx[ci].at[slot, core],
                                          xsem.at[ci, slot, core, 0]).wait()

    lanes = lax.broadcasted_iota(jnp.int32, (t, r), 1)

    def gates(pp, carry):
        src = _chip(c, pp, q) * 2 + c
        meta = meta_ref[src].T
        code = meta[:, :8].astype(jnp.int32)
        for slot in range(4):
            for core in (0, 1):
                base = (_chip(c, p, q + slot) * 2 + core) * r
                gm = jnp.zeros((t, r), F32)
                for i in range(8):
                    gm = gm + jnp.where(code[:, i:i + 1] - base == lanes, meta[:, 8 + i:9 + i], 0.0)
                hi = gm.astype(BF16)
                rest = gm - hi.astype(F32)
                mid = rest.astype(BF16)
                low = (rest - mid.astype(F32)).astype(BF16)
                cols = slice((slot * 2 + core) * r, (slot * 2 + core + 1) * r)
                gs[pp, 0, :, cols] = hi
                gs[pp, 1, :, cols] = mid
                gs[pp, 2, :, cols] = low
        return carry

    def weigh(ci, j, off):
        pp = (p + off) % ND
        w = math.gcd(512, widths[ci])

        def tile(i, carry):
            cols = pl.ds(pl.multiple_of(i * w, w), w)
            rhs = rx[ci][:, :, pp, :, cols].reshape(8 * r, w)
            s = jnp.dot(gs[pp, 0], rhs, preferred_element_type=F32)
            s = s + jnp.dot(gs[pp, 1], rhs, preferred_element_type=F32)
            s = s + jnp.dot(gs[pp, 2], rhs, preferred_element_type=F32)
            acc[ci][j, :, cols] = s
            return carry
        lax.fori_loop(0, widths[ci] // w, tile, 0)

    ends = (_chip(c, p + 1, q) * 2 + c, _chip(c, p + 3, q) * 2 + c)

    def half(i, ci):
        return rcopy(acc[ci].at[0, pl.ds(i * ht, ht)], r2[ci].at[i], psem.at[ci, i], sem2.at[ci, i], ends[i])

    def whole(i, ci):
        return rcopy(acc[ci].at[1 + i], r1[ci].at[i], psem.at[ci, 2 + i], sem1.at[ci, i], ends[i])

    def finalize(ci):
        whole(0, ci).wait_recv()
        whole(1, ci).wait_recv()
        y_ref[:, starts[ci]:starts[ci] + widths[ci]] = (acc[ci][3] + r1[ci][0] + r1[ci][1]).astype(BF16)

    give(0)
    relay(0)
    give(1)
    lax.fori_loop(0, ND, gates, 0)
    for ci in range(nc):
        if ci + 1 < nc:
            relay(ci + 1)
        if ci + 2 < nc:
            give(ci + 2)
        collect(ci)
        weigh(ci, 0, 2)
        half(0, ci).start()
        half(1, ci).start()
        weigh(ci, 1, 1)
        weigh(ci, 2, 3)
        for i in (0, 1):
            half(i, ci).wait_recv()
            own = pl.ds(i * ht, ht)
            acc[ci][1 + i, own] = acc[ci][1 + i, own] + r2[ci][i]
            whole(i, ci).start()
        weigh(ci, 3, 0)
        if ci:
            finalize(ci - 1)
    finalize(nc - 1)
    for ci in range(nc):
        for k in (0, 1):
            for dirn in (0, 1):
                far(k, dirn, ci).wait_send()
                if ci:
                    near(k, dirn, ci).wait_send()
                hop(k, dirn, ci).wait_send()
            pl.when(c != k)(other(k, ci).wait_send)
        for i in (0, 1):
            half(i, ci).wait_send()
            whole(i, ci).wait_send()


def solution(mesh):
    n = mesh.shape['expert']
    assert n == 2 * ND * ND

    def local(x, idx, g, hot_tok, w1, w3, w2):
        t, d = x.shape
        k = idx.shape[1]
        el, _, f = w1.shape
        e = el * n
        ch = hot_tok.shape[0]
        cap = max(ch, 2 * ((t * k - ch + e - 2) // (e - 1)))
        r = el * cap
        widths = [d * i // 16 for i in (8, 8)]
        nc = len(widths)

        hit = idx[:, :, None] == jnp.arange(e, dtype=jnp.int32)
        chosen = hit.any(axis=1).astype(BF16)
        earlier = (jnp.arange(t)[:, None] > jnp.arange(t)[None, :]).astype(BF16)
        before = jnp.dot(earlier, chosen, preferred_element_type=F32)
        rank = jnp.where(hit, before[:, None, :], 0.0).sum(axis=2)
        code = (idx * cap).astype(F32) + rank
        meta = jnp.concatenate([code.T, g.T], axis=0)

        anyspec = pl.BlockSpec(memory_space=pl.ANY)
        vspec = pl.BlockSpec(memory_space=pltpu.VMEM)
        *h, _, metas, near = pl.pallas_call(
            functools.partial(_dispatch_kernel, n, el, cap, nc),
            out_shape=[jax.ShapeDtypeStruct((2, ND, ND, r, w), BF16) for w in widths]
            + [jax.ShapeDtypeStruct((n, t, d), BF16),
               jax.ShapeDtypeStruct((n,) + meta.shape, F32),
               jax.ShapeDtypeStruct((2, 2, ND, r, widths[0]), BF16)],
            in_specs=[anyspec, vspec, anyspec, anyspec, anyspec],
            out_specs=[anyspec] * (nc + 1) + [vspec, anyspec],
            scratch_shapes=[pltpu.VMEM((2, 8 * cap, w), BF16) for w in widths] + [
                pltpu.VMEM(w1.shape, BF16), pltpu.VMEM(w3.shape, BF16), pltpu.VMEM(w2.shape, BF16),
                pltpu.VMEM((8, t, d), BF16), pltpu.VMEM((el, 8 * cap, d), BF16),
                pltpu.VMEM((8 * cap, f), BF16),
                pltpu.SemaphoreType.DMA((3,)), pltpu.SemaphoreType.DMA((8,)), pltpu.SemaphoreType.DMA((2, 8, nc)),
                pltpu.SemaphoreType.DMA((40,)), pltpu.SemaphoreType.DMA((n, 2)),
                pltpu.SemaphoreType.DMA((31,)), pltpu.SemaphoreType.DMA((n,)),
                pltpu.SemaphoreType.DMA((2, 2)), pltpu.SemaphoreType.DMA((2, 2)),
            ],
            compiler_params=pltpu.CompilerParams(collective_id=0, has_side_effects=True,
                                                 vmem_limit_bytes=66_000_000),
        )(x, meta, w1, w3, w2)
        return pl.pallas_call(
            functools.partial(_return_kernel, n, r, nc),
            out_shape=jax.ShapeDtypeStruct((t, d), BF16),
            in_specs=[anyspec] * nc + [vspec, anyspec],
            out_specs=vspec,
            scratch_shapes=[pltpu.VMEM((4, 2, ND, r, w), BF16) for w in widths]
            + [pltpu.VMEM((2, 2, 2, r, w), BF16) for w in widths]
            + [pltpu.VMEM((4, t, w), F32) for w in widths]
            + [pltpu.VMEM((2, t // 2, w), F32) for w in widths]
            + [pltpu.VMEM((2, t, w), F32) for w in widths] + [
                pltpu.VMEM((ND, 3, t, 8 * r), BF16),
                pltpu.SemaphoreType.DMA((nc, 2, 5)), pltpu.SemaphoreType.DMA((nc, 2, 2)),
                pltpu.SemaphoreType.DMA((nc, 4)), pltpu.SemaphoreType.DMA((nc, 4, 2, 2)),
                pltpu.SemaphoreType.DMA((nc, 2, 2)), pltpu.SemaphoreType.DMA((nc, 2)),
                pltpu.SemaphoreType.DMA((nc, 2)),
            ],
            compiler_params=pltpu.CompilerParams(collective_id=1, has_side_effects=True,
                                                 vmem_limit_bytes=60_000_000),
        )(*h, metas, near)

    rows = P(('data', 'expert'))
    wspec = P('expert')
    return jax.shard_map(local, mesh=mesh, in_specs=(rows, rows, rows, rows, wspec, wspec, wspec), out_specs=rows,
                         check_vma=False)
```

```python
import functools
import math

import jax
import jax.numpy as jnp
from jax import lax
from jax.experimental import pallas as pl
from jax.experimental.pallas import tpu as pltpu
from jax.sharding import PartitionSpec as P

MESH = pl.DeviceIdType.MESH
F32 = jnp.float32
BF16 = jnp.bfloat16
ND = 4


def _where(n):
    me = lax.axis_index('expert')
    c = me % 2
    chip = me // 2
    return me, c, chip % ND, chip // ND


def _chip(k, p, q):
    p = p % ND
    q = q % ND
    return (1 - k) * (q * ND + p) + k * (p * ND + q)


def _around(frames):
    return [_chip(k, frames[k][0], frames[k][1] + s) * 2 + core for k in (0, 1) for s in (1, 3) for core in (0, 1)]


def _greet(devs):
    bar = pltpu.get_barrier_semaphore()
    for dev in devs:
        pl.semaphore_signal(bar, inc=1, device_id={'expert': dev}, device_id_type=MESH)
    pl.semaphore_wait(bar, len(devs))


def _dispatch_kernel(n, el, cap, nc, x_ref, idx_ref, g_ref, w1_ref, w3_ref, w2_ref, *refs):
    h_refs, (xall, metas, rn), refs = refs[:nc], refs[nc:nc + 3], refs[nc + 3:]
    hbs, (w1v, w3v, w2v, xb, xg, uv, wsem, bsem, osem, ssem, rsem, msem, mrsem,
          nsem, nrsem) = refs[:nc], refs[nc:]
    t, d = x_ref.shape
    f = w1v.shape[2]
    r = el * cap
    ht = t // 2
    me, c, cx, cy = _where(n)
    o = 1 - c
    p = o * cx + c * cy
    q = o * cy + c * cx
    partner = me + 1 - 2 * c

    def dev(pp, qq):
        return _chip(c, pp, qq) * 2 + c

    pu, pd, qu, qd = dev(p + 1, q), dev(p + 3, q), dev(p, q + 1), dev(p, q + 3)
    frames = ((cx, cy), (cy, cx))
    _greet(_around(frames) + [partner])

    loads = []
    for i, (a, b) in enumerate(((w1_ref, w1v), (w3_ref, w3v), (w2_ref, w2v))):
        loads.append(pltpu.make_async_copy(a, b, wsem.at[i]))
    count = [0, 0]

    def bump(i):
        count[i] += 1
        return count[i] - 1

    def copy(b, ref, half, to, sem):
        rows = pl.ds(0, t) if half is None else pl.ds(half * ht, ht)
        half = half or 0
        return pltpu.make_async_remote_copy(
            src_ref=ref.at[rows], dst_ref=xall.at[b, rows], send_sem=ssem.at[sem], recv_sem=rsem.at[b, half],
            device_id={'expert': to}, device_id_type=MESH)

    def note(b, ref, to, sem):
        return pltpu.make_async_remote_copy(
            src_ref=ref, dst_ref=metas.at[b], send_sem=msem.at[sem], recv_sem=mrsem.at[b],
            device_id={'expert': to}, device_id_type=MESH)

    sizes = []

    def send(b, ref, half, to):
        sizes.append(half)
        copy(b, ref, half, to, bump(0)).start()

    def tell(b, ref, to):
        note(b, ref, to, bump(1)).start()

    def arrived(b, half):
        copy(b, xall.at[b], half, partner, 0).wait_recv()

    def told(b):
        note(b, metas.at[b], partner, 0).wait_recv()

    def take_notes():
        top = idx_ref.shape[0]
        ids = idx_ref[...]
        experts = lax.broadcasted_iota(jnp.int32, (n * el, t), 0)
        hit = experts == ids[0:1, :]
        for j in range(1, top):
            hit = hit | (experts == ids[j:j + 1, :])
        chosen = jnp.where(hit, 1.0, 0.0).astype(BF16)
        earlier = lax.broadcasted_iota(jnp.int32, (t, t), 0) < lax.broadcasted_iota(jnp.int32, (t, t), 1)
        before = jnp.dot(chosen, jnp.where(earlier, 1.0, 0.0).astype(BF16), preferred_element_type=F32)
        row = lax.broadcasted_iota(jnp.int32, (top, t), 0)
        place = ids.astype(F32) * cap
        for j in range(top):
            rank = jnp.sum(jnp.where(experts == ids[j:j + 1, :], before, 0.0), axis=0, keepdims=True)
            place = place + jnp.where(row == j, rank, 0.0)
        metas[me, 0:top] = place
        metas[me, top:2 * top] = g_ref[...]

    for k in (0, 1):
        send(me, x_ref, k, pu)
        send(me, x_ref, 1 - k, pd)
        send(me, x_ref, k, qu)
        send(me, x_ref, 1 - k, qd)
        if k == 0:
            take_notes()
            for to in (pu, pd, qu, qd, partner):
                tell(me, metas.at[me], to)
    send(me, x_ref, None, partner)
    for cp in loads:
        cp.start()

    def spread(b):
        for to in (qu, qd, partner):
            send(b, xall.at[b], None, to)

    def announce(b, *to):
        told(b)
        for to in to:
            tell(b, metas.at[b], to)

    def ring():
        arrived(pd, 0)
        send(pd, xall.at[pd], 0, pu)
        arrived(pu, 1)
        send(pu, xall.at[pu], 1, pd)
        announce(pd, pu, qu, qd, partner)
        announce(pu, qu, qd, partner)
        arrived(pd, 1)
        spread(pd)
        arrived(pu, 0)
        spread(pu)

    def take(dp, dq):
        b = dev(p + dp, q + dq)
        first = 1 if dq == 1 else 0
        on = qd if dq == 1 else qu
        if dq in (1, 3) and dp:
            arrived(b, None)
            send(b, xall.at[b], first, on)
        else:
            arrived(b, first)
            if dq in (1, 3):
                send(b, xall.at[b], first, on)
            arrived(b, 1 - first)
        if dq == 0:
            spread(b)
            announce(b, qu, qd, partner)
            return
        send(b, xall.at[b], None, partner)
        if dq == 3:
            announce(b, qu, partner)
        else:
            announce(b, partner)

    def spot(dp, dq, own):
        if own:
            return c, (p + dp) % ND, (q + dq) % ND
        return o, (q + dp) % ND, (p + dq) % ND

    def source(dp, dq, own):
        k, pp, qq = spot(dp, dq, own)
        return _chip(k, pp, qq) * 2 + k

    rows = lax.broadcasted_iota(jnp.int32, (r, t), 0)
    nf = f // 3
    dt = math.gcd(512, *(hb.shape[-1] for hb in hbs))

    def flush(slot, m):
        for i in range(m):
            for j in range(nc):
                pltpu.make_async_copy(hbs[j].at[slot, pl.ds(i * cap, cap)], h_refs[j].at[0, 0, 0, pl.ds(0, cap)],
                                      osem.at[slot, i, j]).wait()

    def fetch(slot, dp, dq, own):
        src = source(dp, dq, own)
        ref = x_ref if own and dp == 0 and dq == 0 else xall.at[src]
        pltpu.make_async_copy(ref, xb.at[slot], bsem.at[slot]).start()

    def select(slot, dp, dq, own):
        code = metas[source(dp, dq, own)].astype(jnp.int32) - me * r
        hit = rows == code[0:1, :]
        for j in range(1, 8):
            hit = hit | (rows == code[j:j + 1, :])
        sel = jnp.where(hit, 1.0, 0.0).astype(BF16)
        pltpu.make_async_copy(x_ref, xb.at[slot], bsem.at[slot]).wait()
        xs = jnp.dot(sel, xb[slot], preferred_element_type=F32).astype(BF16)
        xg[:, slot * cap:(slot + 1) * cap, :] = xs.reshape(el, cap, d)

    def group(members, before, first=False):
        nb = len(members)
        m = 2 * nb * cap
        for i, (dp, dq) in enumerate(members):
            fetch(i, dp, dq, True)
        for i, (dp, dq) in enumerate(members):
            select(i, dp, dq, True)
        for i, (dp, dq) in enumerate(members):
            src = source(dp, dq, False)
            arrived(src, None)
            told(src)
            fetch(nb + i, dp, dq, False)
        for i, (dp, dq) in enumerate(members):
            select(nb + i, dp, dq, False)
        if first:
            for cp in loads:
                cp.wait()

        def expert(e, carry):
            for i in range(3):
                cols = slice(i * nf, (i + 1) * nf)
                a = jnp.dot(xg[e, 0:m], w1v[e, :, cols], preferred_element_type=F32)
                b = jnp.dot(xg[e, 0:m], w3v[e, :, cols], preferred_element_type=F32)
                uv[0:m, cols] = (a * jax.nn.sigmoid(a) * b).astype(BF16)
            slot = e % 2
            if before == 2 * nb:
                flush(slot, before)
            else:
                pl.when(e >= 2)(lambda: flush(slot, 2 * nb))
                if before:
                    pl.when(e < 2)(lambda: flush(slot, before))
            at = 0
            for hb in hbs:
                for i in range(0, hb.shape[-1], dt):
                    hb[slot, 0:m, i:i + dt] = jnp.dot(uv[0:m], w2v[e, :, at:at + dt],
                                                      preferred_element_type=F32).astype(BF16)
                    at += dt
            for i in range(2 * nb):
                k, pp, qq = spot(*members[i % nb], i < nb)
                for j in range(nc):
                    pltpu.make_async_copy(hbs[j].at[slot, pl.ds(i * cap, cap)],
                                          h_refs[j].at[k, qq, pp, pl.ds(e * cap, cap)], osem.at[slot, i, j]).start()
            return carry
        lax.fori_loop(0, el, expert, 0)
        return 2 * nb

    ring()
    take(0, 1)
    take(0, 3)
    done = group(((0, 0), (1, 0), (3, 0), (0, 1)), 0, True)
    take(2, 0)
    take(3, 1)
    take(3, 3)
    done = group(((0, 3), (2, 0), (3, 1), (3, 3)), done)
    take(1, 1)
    take(1, 3)
    take(2, 1)
    take(2, 3)
    done = group(((1, 1), (1, 3), (2, 1), (2, 3)), done)
    flush(0, done)
    flush(1, done)
    ahead = []
    for k in (0, 1):
        pk, qk = frames[k]
        for dirn, s in ((0, 1), (1, 3)):
            ahead.append(pltpu.make_async_remote_copy(
                src_ref=h_refs[0].at[k, (qk + s) % ND], dst_ref=rn.at[dirn, c], send_sem=nsem.at[k, dirn],
                recv_sem=nrsem.at[dirn, c], device_id={'expert': _chip(k, pk, qk + s) * 2 + k}, device_id_type=MESH))
    for cp in ahead:
        cp.start()
    take(0, 2)
    take(3, 2)
    done = group(((0, 2), (3, 2)), 0)
    take(1, 2)
    take(2, 2)
    done = group(((1, 2), (2, 2)), done)
    flush(0, done)
    flush(1, done)

    for i, half in enumerate(sizes):
        copy(me, x_ref, half, partner, i).wait_send()

    for cp in ahead:
        cp.wait_send()
    for dirn in (0, 1):
        for core in (0, 1):
            pltpu.make_async_remote_copy(
                src_ref=rn.at[dirn, core], dst_ref=rn.at[dirn, core], send_sem=nsem.at[0, 0],
                recv_sem=nrsem.at[dirn, core], device_id={'expert': partner}, device_id_type=MESH).wait_recv()

    def noted(i, carry):
        note(me, metas.at[me], partner, i).wait_send()
        return carry
    lax.fori_loop(0, count[1], noted, 0)
    assert count == [40, 31]


def _return_kernel(n, r, nc, *refs):
    h_refs, (meta_ref, rn, y_ref), refs = refs[:nc], refs[nc:nc + 3], refs[nc + 3:]
    rx, fwd, acc, r2, r1 = (refs[i * nc:(i + 1) * nc] for i in range(5))
    gs, gsem, lsem, psem, xsem, fsem, sem2, sem1 = refs[5 * nc:]
    t, d = y_ref.shape
    widths = [h.shape[-1] for h in h_refs]
    starts = [sum(widths[:i]) for i in range(nc)]
    me, c, cx, cy = _where(n)
    partner = me + 1 - 2 * c
    ht = t // 2
    frames = ((cx, cy), (cy, cx))
    _greet(_around(frames) + [partner])
    o = 1 - c
    p = o * cx + c * cy
    q = o * cy + c * cx

    def rcopy(src, dst, ssem, rsem, to):
        return pltpu.make_async_remote_copy(src_ref=src, dst_ref=dst, send_sem=ssem, recv_sem=rsem,
                                            device_id={'expert': to}, device_id_type=MESH)

    def rows(k, dq, ci):
        return h_refs[ci].at[k, (frames[k][1] + dq) % ND]

    def far(k, dirn, ci):
        pk, qk = frames[k]
        src = h_refs[ci].at[k, (qk + 2) % ND, pl.ds(dirn * 2, 2)]
        return rcopy(src, fwd[ci].at[k, dirn], gsem.at[ci, k, dirn], fsem.at[ci, k, dirn],
                     _chip(k, pk, qk + 1 + 2 * dirn) * 2 + c)

    def near(k, dirn, ci):
        pk, qk = frames[k]
        slot = 3 - 2 * dirn
        return rcopy(rows(k, 1 + 2 * dirn, ci), rx[ci].at[slot, c], gsem.at[ci, k, 2 + dirn],
                     xsem.at[ci, slot, c, 0], _chip(k, pk, qk + 1 + 2 * dirn) * 2 + k)

    def other(k, ci):
        return rcopy(rows(k, 0, ci), rx[ci].at[0, c], gsem.at[ci, k, 4], xsem.at[ci, 0, c, 0], partner)

    def hop(k, dirn, ci):
        pk, qk = frames[k]
        return rcopy(fwd[ci].at[k, dirn], rx[ci].at[2, c, pl.ds(dirn * 2, 2)], lsem.at[ci, k, dirn],
                     xsem.at[ci, 2, c, dirn], _chip(k, pk, qk + 1 + 2 * dirn) * 2 + k)

    def give(ci):
        for k in (0, 1):
            far(k, 0, ci).start()
            far(k, 1, ci).start()
        for k in (0, 1):
            for dirn in (0, 1):
                if ci:
                    near(k, dirn, ci).start()
                else:
                    slot = 3 - 2 * dirn
                    pltpu.make_async_copy(rn.at[dirn, k], rx[0].at[slot, k], xsem.at[0, slot, k, 0]).start()
        for k in (0, 1):
            pl.when(c == k)(pltpu.make_async_copy(rows(k, 0, ci), rx[ci].at[0, c], xsem.at[ci, 0, c, 0]).start)
            pl.when(c != k)(other(k, ci).start)

    def relay(ci):
        for k in (0, 1):
            for dirn in (0, 1):
                far(k, dirn, ci).wait_recv()
                hop(k, dirn, ci).start()

    def collect(ci):
        for slot in range(4):
            for core in (0, 1):
                if slot == 2:
                    for half in (0, 1):
                        two = pl.ds(half * 2, 2)
                        pltpu.make_async_copy(h_refs[ci].at[0, 0, two], rx[ci].at[slot, core, two],
                                              xsem.at[ci, slot, core, half]).wait()
                else:
                    pltpu.make_async_copy(h_refs[ci].at[0, 0], rx[ci].at[slot, core],
                                          xsem.at[ci, slot, core, 0]).wait()

    lanes = lax.broadcasted_iota(jnp.int32, (t, r), 1)

    def gates(pp, carry):
        src = _chip(c, pp, q) * 2 + c
        meta = meta_ref[src].T
        code = meta[:, :8].astype(jnp.int32)
        for slot in range(4):
            for core in (0, 1):
                base = (_chip(c, p, q + slot) * 2 + core) * r
                gm = jnp.zeros((t, r), F32)
                for i in range(8):
                    gm = gm + jnp.where(code[:, i:i + 1] - base == lanes, meta[:, 8 + i:9 + i], 0.0)
                hi = gm.astype(BF16)
                rest = gm - hi.astype(F32)
                mid = rest.astype(BF16)
                low = (rest - mid.astype(F32)).astype(BF16)
                cols = slice((slot * 2 + core) * r, (slot * 2 + core + 1) * r)
                gs[pp, 0, :, cols] = hi
                gs[pp, 1, :, cols] = mid
                gs[pp, 2, :, cols] = low
        return carry

    def weigh(ci, j, off):
        pp = (p + off) % ND
        w = math.gcd(512, widths[ci])

        def tile(i, carry):
            cols = pl.ds(pl.multiple_of(i * w, w), w)
            rhs = rx[ci][:, :, pp, :, cols].reshape(8 * r, w)
            s = jnp.dot(gs[pp, 0], rhs, preferred_element_type=F32)
            s = s + jnp.dot(gs[pp, 1], rhs, preferred_element_type=F32)
            s = s + jnp.dot(gs[pp, 2], rhs, preferred_element_type=F32)
            acc[ci][j, :, cols] = s
            return carry
        lax.fori_loop(0, widths[ci] // w, tile, 0)

    ends = (_chip(c, p + 1, q) * 2 + c, _chip(c, p + 3, q) * 2 + c)

    def half(i, ci):
        return rcopy(acc[ci].at[0, pl.ds(i * ht, ht)], r2[ci].at[i], psem.at[ci, i], sem2.at[ci, i], ends[i])

    def whole(i, ci):
        return rcopy(acc[ci].at[1 + i], r1[ci].at[i], psem.at[ci, 2 + i], sem1.at[ci, i], ends[i])

    def finalize(ci):
        whole(0, ci).wait_recv()
        whole(1, ci).wait_recv()
        y_ref[:, starts[ci]:starts[ci] + widths[ci]] = (acc[ci][3] + r1[ci][0] + r1[ci][1]).astype(BF16)

    give(0)
    relay(0)
    give(1)
    lax.fori_loop(0, ND, gates, 0)
    for ci in range(nc):
        if ci + 1 < nc:
            relay(ci + 1)
        if ci + 2 < nc:
            give(ci + 2)
        collect(ci)
        weigh(ci, 0, 2)
        half(0, ci).start()
        half(1, ci).start()
        weigh(ci, 1, 1)
        weigh(ci, 2, 3)
        for i in (0, 1):
            half(i, ci).wait_recv()
            own = pl.ds(i * ht, ht)
            acc[ci][1 + i, own] = acc[ci][1 + i, own] + r2[ci][i]
            whole(i, ci).start()
        weigh(ci, 3, 0)
        if ci:
            finalize(ci - 1)
    finalize(nc - 1)
    for ci in range(nc):
        for k in (0, 1):
            for dirn in (0, 1):
                far(k, dirn, ci).wait_send()
                if ci:
                    near(k, dirn, ci).wait_send()
                hop(k, dirn, ci).wait_send()
            pl.when(c != k)(other(k, ci).wait_send)
        for i in (0, 1):
            half(i, ci).wait_send()
            whole(i, ci).wait_send()


def solution(mesh):
    n = mesh.shape['expert']
    assert n == 2 * ND * ND

    def local(x, idx, g, hot_tok, w1, w3, w2):
        t, d = x.shape
        k = idx.shape[1]
        el, _, f = w1.shape
        e = el * n
        ch = hot_tok.shape[0]
        cap = max(ch, 2 * ((t * k - ch + e - 2) // (e - 1)))
        r = el * cap
        widths = [d * i // 16 for i in (8, 8)]
        nc = len(widths)

        anyspec = pl.BlockSpec(memory_space=pl.ANY)
        vspec = pl.BlockSpec(memory_space=pltpu.VMEM)
        *h, _, metas, near = pl.pallas_call(
            functools.partial(_dispatch_kernel, n, el, cap, nc),
            out_shape=[jax.ShapeDtypeStruct((2, ND, ND, r, w), BF16) for w in widths]
            + [jax.ShapeDtypeStruct((n, t, d), BF16),
               jax.ShapeDtypeStruct((n, 2 * k, t), F32),
               jax.ShapeDtypeStruct((2, 2, ND, r, widths[0]), BF16)],
            in_specs=[anyspec, vspec, vspec, anyspec, anyspec, anyspec],
            out_specs=[anyspec] * (nc + 1) + [vspec, anyspec],
            scratch_shapes=[pltpu.VMEM((2, 8 * cap, w), BF16) for w in widths] + [
                pltpu.VMEM(w1.shape, BF16), pltpu.VMEM(w3.shape, BF16), pltpu.VMEM(w2.shape, BF16),
                pltpu.VMEM((8, t, d), BF16), pltpu.VMEM((el, 8 * cap, d), BF16),
                pltpu.VMEM((8 * cap, f), BF16),
                pltpu.SemaphoreType.DMA((3,)), pltpu.SemaphoreType.DMA((8,)), pltpu.SemaphoreType.DMA((2, 8, nc)),
                pltpu.SemaphoreType.DMA((40,)), pltpu.SemaphoreType.DMA((n, 2)),
                pltpu.SemaphoreType.DMA((31,)), pltpu.SemaphoreType.DMA((n,)),
                pltpu.SemaphoreType.DMA((2, 2)), pltpu.SemaphoreType.DMA((2, 2)),
            ],
            compiler_params=pltpu.CompilerParams(collective_id=0, has_side_effects=True,
                                                 vmem_limit_bytes=66_000_000),
        )(x, idx.T, g.T, w1, w3, w2)
        return pl.pallas_call(
            functools.partial(_return_kernel, n, r, nc),
            out_shape=jax.ShapeDtypeStruct((t, d), BF16),
            in_specs=[anyspec] * nc + [vspec, anyspec],
            out_specs=vspec,
            scratch_shapes=[pltpu.VMEM((4, 2, ND, r, w), BF16) for w in widths]
            + [pltpu.VMEM((2, 2, 2, r, w), BF16) for w in widths]
            + [pltpu.VMEM((4, t, w), F32) for w in widths]
            + [pltpu.VMEM((2, t // 2, w), F32) for w in widths]
            + [pltpu.VMEM((2, t, w), F32) for w in widths] + [
                pltpu.VMEM((ND, 3, t, 8 * r), BF16),
                pltpu.SemaphoreType.DMA((nc, 2, 5)), pltpu.SemaphoreType.DMA((nc, 2, 2)),
                pltpu.SemaphoreType.DMA((nc, 4)), pltpu.SemaphoreType.DMA((nc, 4, 2, 2)),
                pltpu.SemaphoreType.DMA((nc, 2, 2)), pltpu.SemaphoreType.DMA((nc, 2)),
                pltpu.SemaphoreType.DMA((nc, 2)),
            ],
            compiler_params=pltpu.CompilerParams(collective_id=1, has_side_effects=True,
                                                 vmem_limit_bytes=60_000_000),
        )(*h, metas, near)

    rows = P(('data', 'expert'))
    wspec = P('expert')
    return jax.shard_map(local, mesh=mesh, in_specs=(rows, rows, rows, rows, wspec, wspec, wspec), out_specs=rows,
                         check_vma=False)
```
